32 devices in a mesh: blk: 8 (over y, x, core), grp: 4 (over z).
Axes of the slice: x: 2, y: 2, z: 4, core: 2. Of those that a mesh axis runs over, the one named last changes fastest.
Arguments:
- source: float32 [2048, 128], P(('blk', 'grp')), may hold values from -3 to 3
- target: float32 [2048, 128], P(('blk', 'grp')), may hold values from -3 to 3
- source_mass: float32 [2048], P(('blk', 'grp')), may hold values from 0.25 to 4
- target_mass: float32 [2048], P(('blk', 'grp')), may hold values from 0.25 to 4
Outputs:
- source_dual: float32 [2048], P(('blk', 'grp'))
- target_dual: float32 [2048], P(('blk', 'grp'))
The draws below stay inside these ranges and needn't reach their ends.
All inputs are finite; a program needn't handle non-finite values.
Results may differ from the reference program's by a relative error of at most 0.0003.
Values sent between devices are 32-bit elements; how exact they have to be, the bound alone decides.
No kernel may reach another device: no remote copies, remote signals or barrier semaphores. Data moves between devices by JAX's collectives and lax.ppermute only.
A program may use at most 64 MiB of HBM per device.

```python
import math
import jax
import jax.numpy as jnp
from jax import lax

D = 128
ITERS = 8
POINTS = 2048


def cloud_parts(key):
    cluster_count = max(POINTS // 64, 1)
    centres = jax.random.normal(jax.random.fold_in(key, 3), (cluster_count, D), jnp.float32)
    member = jax.random.randint(jax.random.fold_in(key, 5), (POINTS,), 0, cluster_count)
    spread = jax.random.normal(jax.random.fold_in(key, 7), (POINTS, D), jnp.float32)
    base = 0.11 * centres[member] + 0.1 * spread
    order = jax.random.permutation(jax.random.fold_in(key, 9), POINTS)
    return (base, order)


def far_shift(key):
    picked_count = max(POINTS // 256, 2)
    picks = jax.random.permutation(jax.random.fold_in(key, 19), POINTS)[:picked_count]
    strength = jax.random.uniform(jax.random.fold_in(key, 23), (picked_count,), jnp.float32, 0.85, 1.25)
    flags = jnp.zeros((POINTS,), jnp.float32).at[picks].set(strength)
    return (110.0 / D) ** 0.5 * flags[:, None]


def draw_source(key, part):
    base, order = cloud_parts(key)
    noise = 0.05 * jax.random.normal(jax.random.fold_in(key, 11), (POINTS, D), jnp.float32)
    points = base + noise
    points = points + far_shift(key)
    return jnp.clip(points, -3.0, 3.0)


def draw_target(key, part):
    base, order = cloud_parts(key)
    matched = base[order]
    noise = 0.05 * jax.random.normal(jax.random.fold_in(key, 13), (POINTS, D), jnp.float32)
    return jnp.clip(matched + noise, -3.0, 3.0)


def levels(key, dims, pieces, least, top_value):
    level, own = 1.0, jax.random.fold_in(key, 6)
    for dim, shards_of in pieces:
        heights = jnp.exp(jax.random.uniform(jax.random.fold_in(own, dim), (shards_of,), jnp.float32, least / len(pieces), top_value / len(pieces)))
        level = level * jnp.repeat(heights, dims[dim] // shards_of).reshape([-1 if axis == dim else 1 for axis in range(len(dims))])
    return level


def setup_inputs(seed: int = 0) -> dict:
    key_of = jax.random.split(jax.random.key(seed), 5)
    source = draw_source(jax.random.fold_in(key_of[4], 71), 0)
    target = draw_target(jax.random.fold_in(key_of[4], 71), 0)
    source_mass = jnp.clip(jnp.exp(math.log(4.0) - 2.7725887 * jax.random.uniform(key_of[2], (POINTS,), jnp.float32) ** levels(key_of[2], (POINTS,), ((0, 32),), -0.2, 0.2)), 0.25, 4.0)
    target_mass = jnp.clip(jnp.exp(math.log(4.0) - 2.7725887 * jax.random.uniform(key_of[3], (POINTS,), jnp.float32) ** levels(key_of[3], (POINTS,), ((0, 32),), -0.2, 0.2)), 0.25, 4.0)
    return {"source": source, "target": target, "source_mass": source_mass, "target_mass": target_mass}


eps = 0.5


def half_step(rows, cols, col_dual, col_logmass):
    total = rows.shape[0]
    width = rows.shape[1]
    block = math.gcd(total, 1024)
    col_sq = jnp.sum(cols * cols, axis=1)

    def one_block(piece):
        row_sq = jnp.sum(piece * piece, axis=1)
        inner = lax.dot_general(piece, cols, (((1,), (1,)), ((), ())), precision=lax.Precision.HIGHEST, preferred_element_type=jnp.float32)
        cost = row_sq[:, None] + col_sq[None, :] - 2.0 * inner
        score = col_logmass[None, :] + (col_dual[None, :] - cost) / eps
        top = jnp.max(score, axis=1)
        total_exp = jnp.sum(jnp.exp(score - top[:, None]), axis=1)
        return -eps * (top + jnp.log(total_exp))

    return lax.map(one_block, rows.reshape(total // block, block, width)).reshape(total)


def reference(source, target, source_mass, target_mass):
    log_source = jnp.log(source_mass)
    log_target = jnp.log(target_mass)
    target_dual = jnp.zeros((target.shape[0],), jnp.float32)
    source_dual = jnp.zeros((source.shape[0],), jnp.float32)
    for step in range(ITERS):
        source_dual = half_step(source, target, target_dual, log_target)
        target_dual = half_step(target, source, source_dual, log_source)
    return source_dual, target_dual
```

```python
import functools
import math

import jax
import jax.numpy as jnp
from jax import lax
from jax.experimental import pallas as pl
from jax.experimental.pallas import tpu as pltpu
from jax.sharding import PartitionSpec as P

ITERS = 8


eps = 0.5


def combined_all(value, axis, join):
    pieces = jax.tree.map(lambda part: lax.all_gather(part, axis), value)
    head = jax.tree.map(lambda part: part[0], pieces)
    tail = jax.tree.map(lambda part: part[1:], pieces)
    subtotal, _ = lax.scan(lambda subtotal, piece: (join(subtotal, piece), None), head, tail)
    return subtotal


def partial_sums(rows, cols, col_dual, col_logmass):
    row_sq = jnp.sum(rows * rows, axis=1)
    col_sq = jnp.sum(cols * cols, axis=1)
    inner = lax.dot_general(
        rows,
        cols,
        (((1,), (1,)), ((), ())),
        precision=lax.Precision.HIGHEST,
        preferred_element_type=jnp.float32,
    )
    cost = row_sq[:, None] + col_sq[None, :] - 2.0 * inner
    score = col_logmass[None, :] + (col_dual[None, :] - cost) / eps
    top = jnp.max(score, axis=1)
    total_exp = jnp.sum(jnp.exp(score - top[:, None]), axis=1)
    return (top, total_exp)


def combine_parts(first, second):
    top = jnp.maximum(first[0], second[0])
    total_exp = first[1] * jnp.exp(first[0] - top) + second[1] * jnp.exp(second[0] - top)
    return (top, total_exp)


def spread_dual(dual):
    return lax.all_gather(dual, "grp", axis=0, tiled=True)


def finish(rows, cols, col_dual, col_logmass, count):
    top, total_exp = partial_sums(rows, cols, col_dual, col_logmass)
    top, total_exp = combined_all((top, total_exp), "blk", combine_parts)
    whole = -eps * (top + jnp.log(total_exp))
    return lax.dynamic_slice_in_dim(whole, lax.axis_index("blk") * count, count, 0)


def per_device(source, target, source_mass, target_mass):
    count = source.shape[0]
    log_source = jnp.log(source_mass)
    log_target = jnp.log(target_mass)
    row_side = (
        lax.all_gather(source, "blk", axis=0, tiled=True),
        lax.all_gather(target, "blk", axis=0, tiled=True),
        lax.all_gather(log_source, "blk", axis=0, tiled=True),
        lax.all_gather(log_target, "blk", axis=0, tiled=True),
    )
    col_side = (
        lax.all_gather(source, "grp", axis=0, tiled=True),
        lax.all_gather(target, "grp", axis=0, tiled=True),
        lax.all_gather(log_source, "grp", axis=0, tiled=True),
        lax.all_gather(log_target, "grp", axis=0, tiled=True),
    )
    source_rows, target_rows = (row_side[0], row_side[1])
    source_cols, target_cols, source_logcols, target_logcols = col_side
    target_dual = jnp.zeros((count,), jnp.float32)
    source_dual = jnp.zeros((count,), jnp.float32)
    for step in range(ITERS):
        target_spread = spread_dual(target_dual)
        source_dual = finish(source_rows, target_cols, target_spread, target_logcols, count)
        source_spread = spread_dual(source_dual)
        target_dual = finish(target_rows, source_cols, source_spread, source_logcols, count)
    return (source_dual, target_dual)


LANES = 128
SUB = 8
LOG2E = math.log2(math.e)
KAPPA = LOG2E / eps
FLOOR = 2.0 ** -40
VMEM_BUDGET = 48 * 2**20


def log2(x):
    return jnp.log(x) * LOG2E


def split3(x):
    hi = x.astype(jnp.bfloat16)
    rest = x - hi.astype(jnp.float32)
    mid = rest.astype(jnp.bfloat16)
    lo = (rest - mid.astype(jnp.float32)).astype(jnp.bfloat16)
    return hi, mid, lo


def sinkhorn_kernel(*refs, pieces, n, width):
    ins = refs[:pieces]
    out, stage, left, right, score, plan, mass, fbase, rsum, wref, bref, vref, gref, cref, flags, sems = refs[pieces:]
    total = pieces * n
    copies = [pltpu.make_async_copy(ins[p], stage.at[p], sems.at[p]) for p in range(pieces)]
    for copy in copies:
        copy.start()
    per = LANES // n
    lane = lax.broadcasted_iota(jnp.int32, (1, LANES), 1)
    eye = lax.broadcasted_iota(jnp.int32, (n, LANES), 0) == lax.broadcasted_iota(jnp.int32, (n, LANES), 1)
    for p in range(pieces):
        copies[p].wait()
        hi, mid, lo = split3(stage[p, :n, :] * (2.0 * KAPPA))
        for k, part in enumerate((hi, hi, mid, hi, mid, lo)):
            left[p * n : (p + 1) * n, k * width : (k + 1) * width] = part
        hi, mid, lo = split3(stage[p, n : 2 * n, :])
        for k, part in enumerate((hi, mid, hi, lo, mid, hi)):
            right[p * n : (p + 1) * n, k * width : (k + 1) * width] = part
        mass[p * n : (p + 1) * n, :] = jnp.sum(
            jnp.where(eye, stage[p, 2 * n : 2 * n + 1, :], 0.0), axis=1, keepdims=True
        )
    for q in range(total // LANES):
        b = stage[q * per, 2 * n + 1 : 2 * n + 2, :]
        g = stage[q * per, 2 * n + 2 : 2 * n + 3, :]
        for k in range(1, per):
            b = jnp.where(lane >= k * n, stage[q * per + k, 2 * n + 1 : 2 * n + 2, :], b)
            g = jnp.where(lane >= k * n, stage[q * per + k, 2 * n + 2 : 2 * n + 3, :], g)
        bref[:, q * LANES : (q + 1) * LANES] = jnp.broadcast_to(b, (SUB, LANES))
        gref[:, q * LANES : (q + 1) * LANES] = jnp.broadcast_to(g, (SUB, LANES))

    block = min(total, 256)

    def product(i, carry):
        at = pl.ds(pl.multiple_of(i * block, block), block)
        score[at, :] = lax.dot_general(
            left[at, :], right[...], (((1,), (1,)), ((), ())), preferred_element_type=jnp.float32
        )
        return carry

    lax.fori_loop(0, total // block, product, 0)

    groups = 8
    span = groups * SUB
    zero = jnp.zeros((SUB, total), jnp.float32)

    def settle(colsum):
        c = jnp.broadcast_to(jnp.sum(colsum, axis=0, keepdims=True), (SUB, total))
        cref[...] = c
        return jnp.min(c)

    def accept():
        c = cref[...]
        vref[...] = bref[...] / c
        gref[...] = wref[...] - log2(c)

    flags[0] = 1

    def step(it, carry):
        flags[1] = 0

        @pl.when(flags[0] == 0)
        def scaled():
            def rows(i, state):
                acc, low = state
                base = pl.multiple_of(i * span, span)
                weights = []
                for j in range(groups):
                    at = pl.ds(base + j * SUB, SUB)
                    r = jnp.sum(plan[at, :] * vref[...], axis=1, keepdims=True)
                    low = jnp.minimum(low, r)
                    rsum[at, :] = r
                    weights.append(mass[at, :] / r)
                for j in range(groups):
                    at = pl.ds(base + j * SUB, SUB)
                    acc = acc + plan[at, :] * weights[j]
                return acc, low

            acc, low = lax.fori_loop(0, total // span, rows, (zero, jnp.ones((SUB, 1), jnp.float32)))
            good = (jnp.min(low) >= FLOOR) & (settle(acc) >= FLOOR)
            flags[1] = good.astype(jnp.int32)

            @pl.when(good)
            def _():
                accept()

        @pl.when(flags[1] == 0)
        def absorbed():
            wref[...] = gref[...] + log2(bref[...])

            def rows(i, acc):
                base = pl.multiple_of(i * span, span)
                tops = []
                for j in range(groups):
                    at = pl.ds(base + j * SUB, SUB)
                    tops.append(jnp.max(score[at, :] + wref[...], axis=1, keepdims=True))
                sums = []
                for j in range(groups):
                    at = pl.ds(base + j * SUB, SUB)
                    e = jnp.exp2((score[at, :] + wref[...]) - tops[j])
                    plan[at, :] = e
                    sums.append(jnp.sum(e, axis=1, keepdims=True))
                for j in range(groups):
                    at = pl.ds(base + j * SUB, SUB)
                    fbase[at, :] = -(tops[j] + log2(sums[j]))
                    rsum[at, :] = jnp.ones((SUB, 1), jnp.float32)
                    k = plan[at, :] * (1.0 / sums[j])
                    plan[at, :] = k
                    acc = acc + k * mass[at, :]
                return acc

            good = settle(lax.fori_loop(0, total // span, rows, zero)) >= FLOOR
            flags[0] = 1 - good.astype(jnp.int32)

            @pl.when(good)
            def _():
                accept()

            @pl.when(jnp.logical_not(good))
            def columns():
                def top_of(i, top):
                    at = pl.ds(pl.multiple_of(i * SUB, SUB), SUB)
                    return jnp.maximum(top, score[at, :] + (log2(mass[at, :]) + fbase[at, :]))

                top = lax.fori_loop(0, total // SUB, top_of, jnp.full((SUB, total), -jnp.inf, jnp.float32))
                cref[...] = jnp.broadcast_to(jnp.max(top, axis=0, keepdims=True), (SUB, total))

                def sum_of(i, acc):
                    at = pl.ds(pl.multiple_of(i * SUB, SUB), SUB)
                    return acc + jnp.exp2((score[at, :] + (log2(mass[at, :]) + fbase[at, :])) - cref[...])

                acc = jnp.sum(lax.fori_loop(0, total // SUB, sum_of, zero), axis=0, keepdims=True)
                gref[...] = jnp.broadcast_to(-(cref[:1, :] + log2(acc)), (SUB, total))

        return carry

    lax.fori_loop(0, ITERS, step, 0)
    f = fbase[:n, :] - log2(rsum[:n, :])
    f = jnp.sum(jnp.where(eye, f, 0.0), axis=0, keepdims=True)
    out[...] = jnp.zeros(out.shape, jnp.float32)
    out[0:1, :] = f * (1.0 / KAPPA) + stage[0, 2 * n + 3 : 2 * n + 4, :]
    out[1:2, :] = gref[0:1, :LANES] * (1.0 / KAPPA) + stage[0, 2 * n + 4 : 2 * n + 5, :]


def shifts(blk, grp, flip, turn):
    return [
        (b * grp + g, (b ^ flip) * grp + (g + turn) % grp) for b in range(blk) for g in range(grp)
    ]


def replicated(blk, grp, source, target, source_mass, target_mass):
    n, width = source.shape
    axes = ("blk", "grp")
    pieces = blk * grp
    total = pieces * n
    source_sq = jnp.sum(source * source, axis=1)
    target_sq = jnp.sum(target * target, axis=1)
    lines = jnp.stack([source_mass, target_mass, -KAPPA * target_sq, source_sq, target_sq])
    lines = jnp.pad(jnp.tile(lines, (1, LANES // n)), ((0, SUB - lines.shape[0]), (0, 0)))
    own = jnp.concatenate([source, target, lines], axis=0)
    have = [own]
    have = have + [lax.ppermute(own, axes, shifts(blk, grp, 0, turn)) for turn in range(1, grp)]
    for flip in range(2, blk, 2):
        have = have + [lax.ppermute(part, axes, shifts(blk, grp, flip, 0)) for part in have[:grp]]
    have = have + [lax.ppermute(part, axes, shifts(blk, grp, 1, 0)) for part in have]
    rows = own.shape[0]
    f32 = jnp.float32
    column = pltpu.VMEM((total, 1), f32)
    line = pltpu.VMEM((SUB, total), f32)
    duals = pl.pallas_call(
        functools.partial(sinkhorn_kernel, pieces=pieces, n=n, width=width),
        in_specs=[pl.BlockSpec(memory_space=pl.ANY)] * pieces,
        out_specs=pl.BlockSpec(memory_space=pltpu.VMEM),
        out_shape=jax.ShapeDtypeStruct((SUB, LANES), f32),
        scratch_shapes=[
            pltpu.VMEM((pieces, rows, width), f32),
            pltpu.VMEM((total, 6 * width), jnp.bfloat16),
            pltpu.VMEM((total, 6 * width), jnp.bfloat16),
            pltpu.VMEM((total, total), f32),
            pltpu.VMEM((total, total), f32),
            column,
            column,
            column,
            line,
            line,
            line,
            line,
            line,
            pltpu.SMEM((2,), jnp.int32),
            pltpu.SemaphoreType.DMA((pieces,)),
        ],
        compiler_params=pltpu.CompilerParams(vmem_limit_bytes=60 * 2**20),
        name="sinkhorn",
    )(*have)
    return duals[0, :n], duals[1, :n]


def fits(mesh, n, width):
    blk, grp = mesh.shape["blk"], mesh.shape["grp"]
    total = blk * grp * n
    held = 8 * total * total + 32 * total * width
    return width == LANES and LANES % n == 0 and n % SUB == 0 and total % 256 == 0 and blk & (blk - 1) == 0 and blk > 1 and held <= VMEM_BUDGET


def solution(mesh):
    def body(source, target, source_mass, target_mass):
        if fits(mesh, *source.shape):
            return replicated(mesh.shape["blk"], mesh.shape["grp"], source, target, source_mass, target_mass)
        return per_device(source, target, source_mass, target_mass)

    return jax.shard_map(
        body,
        mesh=mesh,
        in_specs=(
            P(("blk", "grp"), None),
            P(("blk", "grp"), None),
            P(("blk", "grp")),
            P(("blk", "grp")),
        ),
        out_specs=(P(("blk", "grp")), P(("blk", "grp"))),
        check_vma=False,
    )
```

```python
import functools
import math

import jax
import jax.numpy as jnp
from jax import lax
from jax.experimental import pallas as pl
from jax.experimental.pallas import tpu as pltpu
from jax.sharding import PartitionSpec as P

ITERS = 8


eps = 0.5


def combined_all(value, axis, join):
    pieces = jax.tree.map(lambda part: lax.all_gather(part, axis), value)
    head = jax.tree.map(lambda part: part[0], pieces)
    tail = jax.tree.map(lambda part: part[1:], pieces)
    subtotal, _ = lax.scan(lambda subtotal, piece: (join(subtotal, piece), None), head, tail)
    return subtotal


def partial_sums(rows, cols, col_dual, col_logmass):
    row_sq = jnp.sum(rows * rows, axis=1)
    col_sq = jnp.sum(cols * cols, axis=1)
    inner = lax.dot_general(
        rows,
        cols,
        (((1,), (1,)), ((), ())),
        precision=lax.Precision.HIGHEST,
        preferred_element_type=jnp.float32,
    )
    cost = row_sq[:, None] + col_sq[None, :] - 2.0 * inner
    score = col_logmass[None, :] + (col_dual[None, :] - cost) / eps
    top = jnp.max(score, axis=1)
    total_exp = jnp.sum(jnp.exp(score - top[:, None]), axis=1)
    return (top, total_exp)


def combine_parts(first, second):
    top = jnp.maximum(first[0], second[0])
    total_exp = first[1] * jnp.exp(first[0] - top) + second[1] * jnp.exp(second[0] - top)
    return (top, total_exp)


def spread_dual(dual):
    return lax.all_gather(dual, "grp", axis=0, tiled=True)


def finish(rows, cols, col_dual, col_logmass, count):
    top, total_exp = partial_sums(rows, cols, col_dual, col_logmass)
    top, total_exp = combined_all((top, total_exp), "blk", combine_parts)
    whole = -eps * (top + jnp.log(total_exp))
    return lax.dynamic_slice_in_dim(whole, lax.axis_index("blk") * count, count, 0)


def per_device(source, target, source_mass, target_mass):
    count = source.shape[0]
    log_source = jnp.log(source_mass)
    log_target = jnp.log(target_mass)
    row_side = (
        lax.all_gather(source, "blk", axis=0, tiled=True),
        lax.all_gather(target, "blk", axis=0, tiled=True),
        lax.all_gather(log_source, "blk", axis=0, tiled=True),
        lax.all_gather(log_target, "blk", axis=0, tiled=True),
    )
    col_side = (
        lax.all_gather(source, "grp", axis=0, tiled=True),
        lax.all_gather(target, "grp", axis=0, tiled=True),
        lax.all_gather(log_source, "grp", axis=0, tiled=True),
        lax.all_gather(log_target, "grp", axis=0, tiled=True),
    )
    source_rows, target_rows = (row_side[0], row_side[1])
    source_cols, target_cols, source_logcols, target_logcols = col_side
    target_dual = jnp.zeros((count,), jnp.float32)
    source_dual = jnp.zeros((count,), jnp.float32)
    for step in range(ITERS):
        target_spread = spread_dual(target_dual)
        source_dual = finish(source_rows, target_cols, target_spread, target_logcols, count)
        source_spread = spread_dual(source_dual)
        target_dual = finish(target_rows, source_cols, source_spread, source_logcols, count)
    return (source_dual, target_dual)


LANES = 128
SUB = 8
LOG2E = math.log2(math.e)
KAPPA = LOG2E / eps
FLOOR = 2.0 ** -40
VMEM_BUDGET = 48 * 2**20
BLOCK = 1024
GROUPS = 16


def log2(x):
    return jnp.log(x) * LOG2E


def split3(x):
    hi = x.astype(jnp.bfloat16)
    rest = x - hi.astype(jnp.float32)
    mid = rest.astype(jnp.bfloat16)
    lo = (rest - mid.astype(jnp.float32)).astype(jnp.bfloat16)
    return hi, mid, lo


def sinkhorn_kernel(*refs, pieces, n, width):
    ins = refs[:pieces]
    out, stage, left, right, score, plan, mass, fbase, rsum, wref, bref, vref, gref, cref, flags, sems = refs[pieces:]
    total = pieces * n
    copies = [pltpu.make_async_copy(ins[p], stage.at[p], sems.at[p]) for p in range(pieces)]
    for copy in copies:
        copy.start()
    per = LANES // n
    lane = lax.broadcasted_iota(jnp.int32, (1, LANES), 1)
    eye = lax.broadcasted_iota(jnp.int32, (n, LANES), 0) == lax.broadcasted_iota(jnp.int32, (n, LANES), 1)
    for p in range(pieces):
        copies[p].wait()
        hi, mid, lo = split3(stage[p, :n, :] * (2.0 * KAPPA))
        for k, part in enumerate((hi, hi, mid, hi, mid, lo)):
            left[p * n : (p + 1) * n, k * width : (k + 1) * width] = part
        hi, mid, lo = split3(stage[p, n : 2 * n, :])
        for k, part in enumerate((hi, mid, hi, lo, mid, hi)):
            right[p * n : (p + 1) * n, k * width : (k + 1) * width] = part
        own = jnp.sum(jnp.where(eye, stage[p, 2 * n : 2 * n + 1, :], 0.0), axis=1, keepdims=True)
        mass[p * n : (p + 1) * n, :] = jnp.broadcast_to(own, (n, LANES))
    for q in range(total // LANES):
        b = stage[q * per, 2 * n + 1 : 2 * n + 2, :]
        g = stage[q * per, 2 * n + 2 : 2 * n + 3, :]
        for k in range(1, per):
            b = jnp.where(lane >= k * n, stage[q * per + k, 2 * n + 1 : 2 * n + 2, :], b)
            g = jnp.where(lane >= k * n, stage[q * per + k, 2 * n + 2 : 2 * n + 3, :], g)
        bref[:, q * LANES : (q + 1) * LANES] = jnp.broadcast_to(b, (SUB, LANES))
        gref[:, q * LANES : (q + 1) * LANES] = jnp.broadcast_to(g, (SUB, LANES))

    block = min(total, BLOCK)

    def product(i, carry):
        at = pl.ds(pl.multiple_of(i * block, block), block)
        part = lax.dot_general(
            left[at, :], right[...], (((1,), (1,)), ((), ())), preferred_element_type=jnp.float32
        )
        score[at, :] = part
        return carry

    lax.fori_loop(0, total // block, product, 0)

    span = GROUPS * SUB
    steps = total // span
    tiles = [slice(c * LANES, (c + 1) * LANES) for c in range(total // LANES)]
    wide = (SUB, LANES)

    def ranges(i):
        base = pl.multiple_of(i * span, span)
        return [pl.ds(base + j * SUB, SUB) for j in range(GROUPS)]

    def spread(column):
        return jnp.broadcast_to(column, wide)

    def settle():
        low = None
        for c in tiles:
            col = jnp.broadcast_to(jnp.sum(cref[:, c], axis=0, keepdims=True), wide)
            cref[:, c] = col
            low = col if low is None else jnp.minimum(low, col)
        return jnp.min(low)

    def accept():
        for c in tiles:
            col = cref[:, c]
            vref[:, c] = bref[:, c] / col
            gref[:, c] = wref[:, c] - log2(col)

    def accumulate(i, weights):
        at = ranges(i)
        for c in tiles:
            acc = [plan[at[j], c] * weights[j] for j in range(GROUPS)]
            while len(acc) > 1:
                acc = [x + y for x, y in zip(acc[::2], acc[1::2])]
            cref[:, c] = cref[:, c] + acc[0]

    def sweep(sums_of):
        cref[...] = jnp.zeros((SUB, total), jnp.float32)

        def weigh(i, low):
            at = ranges(i)
            sums = sums_of(at)
            weights = []
            for j in range(GROUPS):
                rsum[at[j], :] = sums[j]
                low = jnp.minimum(low, sums[j])
                weights.append(mass[at[j], :] / sums[j])
            return low, weights

        def body(i, state):
            low, weights = state
            low, fresh = weigh(i, low)
            accumulate(i - 1, weights)
            return low, fresh

        state = weigh(0, jnp.ones(wide, jnp.float32))
        low, weights = lax.fori_loop(1, steps, body, state)
        accumulate(steps - 1, weights)
        return (jnp.min(low) >= FLOOR) & (settle() >= FLOOR)

    flags[0] = 1

    def step(it, carry):
        flags[1] = 0

        @pl.when(flags[0] == 0)
        def scaled():
            def sums_of(at):
                acc = [None] * GROUPS
                for c in tiles:
                    v = vref[:, c]
                    for j in range(GROUPS):
                        term = plan[at[j], c] * v
                        acc[j] = term if acc[j] is None else acc[j] + term
                return [spread(jnp.sum(x, axis=1, keepdims=True)) for x in acc]

            good = sweep(sums_of)
            flags[1] = good.astype(jnp.int32)

            @pl.when(good)
            def _():
                accept()

        @pl.when(flags[1] == 0)
        def absorbed():
            wref[...] = gref[...] + log2(bref[...])

            def tops(i, carry):
                at = ranges(i)
                best = [None] * GROUPS
                for c in tiles:
                    w = wref[:, c]
                    for j in range(GROUPS):
                        term = score[at[j], c] + w
                        best[j] = term if best[j] is None else jnp.maximum(best[j], term)
                for j in range(GROUPS):
                    fbase[at[j], :] = -spread(jnp.max(best[j], axis=1, keepdims=True))
                return carry

            lax.fori_loop(0, steps, tops, 0)

            def sums_of(at):
                acc = [None] * GROUPS
                low = [fbase[at[j], :] for j in range(GROUPS)]
                for c in tiles:
                    w = wref[:, c]
                    for j in range(GROUPS):
                        term = jnp.exp2((score[at[j], c] + w) + low[j])
                        plan[at[j], c] = term
                        acc[j] = term if acc[j] is None else acc[j] + term
                return [spread(jnp.sum(x, axis=1, keepdims=True)) for x in acc]

            good = sweep(sums_of)
            flags[0] = 1 - good.astype(jnp.int32)

            @pl.when(good)
            def _():
                accept()

            @pl.when(jnp.logical_not(good))
            def columns():
                def height(at):
                    return (log2(mass[at, :1]) + fbase[at, :1]) - log2(rsum[at, :1])

                def top_of(i, top):
                    at = pl.ds(pl.multiple_of(i * SUB, SUB), SUB)
                    return jnp.maximum(top, score[at, :] + height(at))

                top = lax.fori_loop(0, total // SUB, top_of, jnp.full((SUB, total), -jnp.inf, jnp.float32))
                cref[...] = jnp.broadcast_to(jnp.max(top, axis=0, keepdims=True), (SUB, total))

                def sum_of(i, acc):
                    at = pl.ds(pl.multiple_of(i * SUB, SUB), SUB)
                    return acc + jnp.exp2((score[at, :] + height(at)) - cref[...])

                acc = lax.fori_loop(0, total // SUB, sum_of, jnp.zeros((SUB, total), jnp.float32))
                acc = jnp.sum(acc, axis=0, keepdims=True)
                gref[...] = jnp.broadcast_to(-(cref[:1, :] + log2(acc)), (SUB, total))

        return carry

    lax.fori_loop(0, ITERS, step, 0)
    f = fbase[:n, :] - log2(rsum[:n, :])
    f = jnp.sum(jnp.where(eye, f, 0.0), axis=0, keepdims=True)
    out[...] = jnp.zeros(out.shape, jnp.float32)
    out[0:1, :] = f * (1.0 / KAPPA) + stage[0, 2 * n + 3 : 2 * n + 4, :]
    out[1:2, :] = gref[0:1, :LANES] * (1.0 / KAPPA) + stage[0, 2 * n + 4 : 2 * n + 5, :]


def shifts(blk, grp, flip, turn):
    return [
        (b * grp + g, (b ^ flip) * grp + (g + turn) % grp) for b in range(blk) for g in range(grp)
    ]


def replicated(blk, grp, source, target, source_mass, target_mass):
    n, width = source.shape
    axes = ("blk", "grp")
    pieces = blk * grp
    total = pieces * n
    source_sq = jnp.sum(source * source, axis=1)
    target_sq = jnp.sum(target * target, axis=1)
    lines = jnp.stack([source_mass, target_mass, -KAPPA * target_sq, source_sq, target_sq])
    lines = jnp.pad(jnp.tile(lines, (1, LANES // n)), ((0, SUB - lines.shape[0]), (0, 0)))
    own = jnp.concatenate([source, target, lines], axis=0)
    have = [own]
    have = have + [lax.ppermute(own, axes, shifts(blk, grp, 0, turn)) for turn in range(1, grp)]
    for flip in range(2, blk, 2):
        have = have + [lax.ppermute(part, axes, shifts(blk, grp, flip, 0)) for part in have[:grp]]
    have = have + [lax.ppermute(part, axes, shifts(blk, grp, 1, 0)) for part in have]
    rows = own.shape[0]
    f32 = jnp.float32
    column = pltpu.VMEM((total, LANES), f32)
    line = pltpu.VMEM((SUB, total), f32)
    duals = pl.pallas_call(
        functools.partial(sinkhorn_kernel, pieces=pieces, n=n, width=width),
        in_specs=[pl.BlockSpec(memory_space=pl.ANY)] * pieces,
        out_specs=pl.BlockSpec(memory_space=pltpu.VMEM),
        out_shape=jax.ShapeDtypeStruct((SUB, LANES), f32),
        scratch_shapes=[
            pltpu.VMEM((pieces, rows, width), f32),
            pltpu.VMEM((total, 6 * width), jnp.bfloat16),
            pltpu.VMEM((total, 6 * width), jnp.bfloat16),
            pltpu.VMEM((total, total), f32),
            pltpu.VMEM((total, total), f32),
            column,
            column,
            column,
            line,
            line,
            line,
            line,
            line,
            pltpu.SMEM((2,), jnp.int32),
            pltpu.SemaphoreType.DMA((pieces,)),
        ],
        compiler_params=pltpu.CompilerParams(vmem_limit_bytes=60 * 2**20),
        name="sinkhorn",
    )(*have)
    return duals[0, :n], duals[1, :n]


def fits(mesh, n, width):
    blk, grp = mesh.shape["blk"], mesh.shape["grp"]
    total = blk * grp * n
    held = 8 * total * total + 32 * total * width
    return width == LANES and LANES % n == 0 and n % SUB == 0 and total % 256 == 0 and blk & (blk - 1) == 0 and blk > 1 and held <= VMEM_BUDGET


def solution(mesh):
    def body(source, target, source_mass, target_mass):
        if fits(mesh, *source.shape):
            return replicated(mesh.shape["blk"], mesh.shape["grp"], source, target, source_mass, target_mass)
        return per_device(source, target, source_mass, target_mass)

    return jax.shard_map(
        body,
        mesh=mesh,
        in_specs=(
            P(("blk", "grp"), None),
            P(("blk", "grp"), None),
            P(("blk", "grp")),
            P(("blk", "grp")),
        ),
        out_specs=(P(("blk", "grp")), P(("blk", "grp"))),
        check_vma=False,
    )
```

```python
import functools
import math

import jax
import jax.numpy as jnp
from jax import lax
from jax.experimental import pallas as pl
from jax.experimental.pallas import tpu as pltpu
from jax.sharding import PartitionSpec as P

ITERS = 8


eps = 0.5


def combined_all(value, axis, join):
    pieces = jax.tree.map(lambda part: lax.all_gather(part, axis), value)
    head = jax.tree.map(lambda part: part[0], pieces)
    tail = jax.tree.map(lambda part: part[1:], pieces)
    subtotal, _ = lax.scan(lambda subtotal, piece: (join(subtotal, piece), None), head, tail)
    return subtotal


def partial_sums(rows, cols, col_dual, col_logmass):
    row_sq = jnp.sum(rows * rows, axis=1)
    col_sq = jnp.sum(cols * cols, axis=1)
    inner = lax.dot_general(
        rows,
        cols,
        (((1,), (1,)), ((), ())),
        precision=lax.Precision.HIGHEST,
        preferred_element_type=jnp.float32,
    )
    cost = row_sq[:, None] + col_sq[None, :] - 2.0 * inner
    score = col_logmass[None, :] + (col_dual[None, :] - cost) / eps
    top = jnp.max(score, axis=1)
    total_exp = jnp.sum(jnp.exp(score - top[:, None]), axis=1)
    return (top, total_exp)


def combine_parts(first, second):
    top = jnp.maximum(first[0], second[0])
    total_exp = first[1] * jnp.exp(first[0] - top) + second[1] * jnp.exp(second[0] - top)
    return (top, total_exp)


def spread_dual(dual):
    return lax.all_gather(dual, "grp", axis=0, tiled=True)


def finish(rows, cols, col_dual, col_logmass, count):
    top, total_exp = partial_sums(rows, cols, col_dual, col_logmass)
    top, total_exp = combined_all((top, total_exp), "blk", combine_parts)
    whole = -eps * (top + jnp.log(total_exp))
    return lax.dynamic_slice_in_dim(whole, lax.axis_index("blk") * count, count, 0)


def per_device(source, target, source_mass, target_mass):
    count = source.shape[0]
    log_source = jnp.log(source_mass)
    log_target = jnp.log(target_mass)
    row_side = (
        lax.all_gather(source, "blk", axis=0, tiled=True),
        lax.all_gather(target, "blk", axis=0, tiled=True),
        lax.all_gather(log_source, "blk", axis=0, tiled=True),
        lax.all_gather(log_target, "blk", axis=0, tiled=True),
    )
    col_side = (
        lax.all_gather(source, "grp", axis=0, tiled=True),
        lax.all_gather(target, "grp", axis=0, tiled=True),
        lax.all_gather(log_source, "grp", axis=0, tiled=True),
        lax.all_gather(log_target, "grp", axis=0, tiled=True),
    )
    source_rows, target_rows = (row_side[0], row_side[1])
    source_cols, target_cols, source_logcols, target_logcols = col_side
    target_dual = jnp.zeros((count,), jnp.float32)
    source_dual = jnp.zeros((count,), jnp.float32)
    for step in range(ITERS):
        target_spread = spread_dual(target_dual)
        source_dual = finish(source_rows, target_cols, target_spread, target_logcols, count)
        source_spread = spread_dual(source_dual)
        target_dual = finish(target_rows, source_cols, source_spread, source_logcols, count)
    return (source_dual, target_dual)


LANES = 128
SUB = 8
LOG2E = math.log2(math.e)
KAPPA = LOG2E / eps
FLOOR = 2.0 ** -40
VMEM_BUDGET = 48 * 2**20
BLOCK = 1024
GROUPS = 16


def log2(x):
    return jnp.log(x) * LOG2E


def split3(x):
    hi = x.astype(jnp.bfloat16)
    rest = x - hi.astype(jnp.float32)
    mid = rest.astype(jnp.bfloat16)
    lo = (rest - mid.astype(jnp.float32)).astype(jnp.bfloat16)
    return hi, mid, lo


def sinkhorn_kernel(*refs, pieces, n, width):
    out, stage, left, right, score, plan, mass, fbase, rsum, wref, bref, vref, gref, cref, flags, sems = refs[-16:]
    ins = refs[:-16]
    total = pieces * n
    per_group = pieces // len(ins)
    copies = [
        pltpu.make_async_copy(part, stage.at[pl.ds(k * per_group, per_group)], sems.at[k])
        for k, part in enumerate(ins)
    ]
    for copy in copies:
        copy.start()
    per = LANES // n
    lane = lax.broadcasted_iota(jnp.int32, (1, LANES), 1)
    eye = lax.broadcasted_iota(jnp.int32, (n, LANES), 0) == lax.broadcasted_iota(jnp.int32, (n, LANES), 1)
    for p in range(pieces):
        if p % per_group == 0:
            copies[p // per_group].wait()
        hi, mid, lo = split3(stage[p, :n, :] * (2.0 * KAPPA))
        for k, part in enumerate((hi, hi, mid, hi, mid, lo)):
            left[p * n : (p + 1) * n, k * width : (k + 1) * width] = part
        hi, mid, lo = split3(stage[p, n : 2 * n, :])
        for k, part in enumerate((hi, mid, hi, lo, mid, hi)):
            right[p * n : (p + 1) * n, k * width : (k + 1) * width] = part
        own = jnp.sum(jnp.where(eye, stage[p, 2 * n : 2 * n + 1, :], 0.0), axis=1, keepdims=True)
        mass[p * n : (p + 1) * n, :] = jnp.broadcast_to(own, (n, LANES))
    for q in range(total // LANES):
        b = stage[q * per, 2 * n + 1 : 2 * n + 2, :]
        g = stage[q * per, 2 * n + 2 : 2 * n + 3, :]
        for k in range(1, per):
            b = jnp.where(lane >= k * n, stage[q * per + k, 2 * n + 1 : 2 * n + 2, :], b)
            g = jnp.where(lane >= k * n, stage[q * per + k, 2 * n + 2 : 2 * n + 3, :], g)
        bref[:, q * LANES : (q + 1) * LANES] = jnp.broadcast_to(b, (SUB, LANES))
        gref[:, q * LANES : (q + 1) * LANES] = jnp.broadcast_to(g, (SUB, LANES))

    block = min(total, BLOCK)

    def product(i, carry):
        at = pl.ds(pl.multiple_of(i * block, block), block)
        part = lax.dot_general(
            left[at, :], right[...], (((1,), (1,)), ((), ())), preferred_element_type=jnp.float32
        )
        score[at, :] = part
        return carry

    lax.fori_loop(0, total // block, product, 0)

    span = GROUPS * SUB
    steps = total // span
    tiles = [slice(c * LANES, (c + 1) * LANES) for c in range(total // LANES)]
    wide = (SUB, LANES)

    def ranges(i):
        base = pl.multiple_of(i * span, span)
        return [pl.ds(base + j * SUB, SUB) for j in range(GROUPS)]

    def spread(column):
        return jnp.broadcast_to(column, wide)

    def settle():
        low = None
        for c in tiles:
            col = jnp.broadcast_to(jnp.sum(cref[:, c], axis=0, keepdims=True), wide)
            cref[:, c] = col
            low = col if low is None else jnp.minimum(low, col)
        return jnp.min(low)

    def accept():
        for c in tiles:
            col = cref[:, c]
            vref[:, c] = bref[:, c] / col
            gref[:, c] = wref[:, c] - log2(col)

    def accumulate(i, weights):
        at = ranges(i)
        for c in tiles:
            acc = [plan[at[j], c] * weights[j] for j in range(GROUPS)]
            while len(acc) > 1:
                acc = [x + y for x, y in zip(acc[::2], acc[1::2])]
            cref[:, c] = cref[:, c] + acc[0]

    def sweep(sums_of):
        cref[...] = jnp.zeros((SUB, total), jnp.float32)

        def weigh(i, low):
            at = ranges(i)
            sums = sums_of(at)
            weights = []
            for j in range(GROUPS):
                rsum[at[j], :] = sums[j]
                low = jnp.minimum(low, sums[j])
                weights.append(mass[at[j], :] / sums[j])
            return low, weights

        def body(i, state):
            low, weights = state
            low, fresh = weigh(i, low)
            accumulate(i - 1, weights)
            return low, fresh

        state = weigh(0, jnp.ones(wide, jnp.float32))
        low, weights = lax.fori_loop(1, steps, body, state)
        accumulate(steps - 1, weights)
        return (jnp.min(low) >= FLOOR) & (settle() >= FLOOR)

    flags[0] = 1

    def step(it, carry):
        flags[1] = 0

        @pl.when(flags[0] == 0)
        def scaled():
            def sums_of(at):
                acc = [None] * GROUPS
                for c in tiles:
                    v = vref[:, c]
                    for j in range(GROUPS):
                        term = plan[at[j], c] * v
                        acc[j] = term if acc[j] is None else acc[j] + term
                return [spread(jnp.sum(x, axis=1, keepdims=True)) for x in acc]

            good = sweep(sums_of)
            flags[1] = good.astype(jnp.int32)

            @pl.when(good)
            def _():
                accept()

        @pl.when(flags[1] == 0)
        def absorbed():
            wref[...] = gref[...] + log2(bref[...])

            def tops(i, carry):
                at = ranges(i)
                best = [None] * GROUPS
                for c in tiles:
                    w = wref[:, c]
                    for j in range(GROUPS):
                        term = score[at[j], c] + w
                        best[j] = term if best[j] is None else jnp.maximum(best[j], term)
                for j in range(GROUPS):
                    fbase[at[j], :] = -spread(jnp.max(best[j], axis=1, keepdims=True))
                return carry

            lax.fori_loop(0, steps, tops, 0)

            def sums_of(at):
                acc = [None] * GROUPS
                low = [fbase[at[j], :] for j in range(GROUPS)]
                for c in tiles:
                    w = wref[:, c]
                    for j in range(GROUPS):
                        term = jnp.exp2((score[at[j], c] + w) + low[j])
                        plan[at[j], c] = term
                        acc[j] = term if acc[j] is None else acc[j] + term
                return [spread(jnp.sum(x, axis=1, keepdims=True)) for x in acc]

            good = sweep(sums_of)
            flags[0] = 1 - good.astype(jnp.int32)

            @pl.when(good)
            def _():
                accept()

            @pl.when(jnp.logical_not(good))
            def columns():
                def height(at):
                    return (log2(mass[at, :1]) + fbase[at, :1]) - log2(rsum[at, :1])

                def top_of(i, top):
                    at = pl.ds(pl.multiple_of(i * SUB, SUB), SUB)
                    return jnp.maximum(top, score[at, :] + height(at))

                top = lax.fori_loop(0, total // SUB, top_of, jnp.full((SUB, total), -jnp.inf, jnp.float32))
                cref[...] = jnp.broadcast_to(jnp.max(top, axis=0, keepdims=True), (SUB, total))

                def sum_of(i, acc):
                    at = pl.ds(pl.multiple_of(i * SUB, SUB), SUB)
                    return acc + jnp.exp2((score[at, :] + height(at)) - cref[...])

                acc = lax.fori_loop(0, total // SUB, sum_of, jnp.zeros((SUB, total), jnp.float32))
                acc = jnp.sum(acc, axis=0, keepdims=True)
                gref[...] = jnp.broadcast_to(-(cref[:1, :] + log2(acc)), (SUB, total))

        return carry

    lax.fori_loop(0, ITERS, step, 0)
    f = fbase[:n, :] - log2(rsum[:n, :])
    f = jnp.sum(jnp.where(eye, f, 0.0), axis=0, keepdims=True)
    out[...] = jnp.zeros(out.shape, jnp.float32)
    out[0:1, :] = f * (1.0 / KAPPA) + stage[0, 2 * n + 3 : 2 * n + 4, :]
    out[1:2, :] = gref[0:1, :LANES] * (1.0 / KAPPA) + stage[0, 2 * n + 4 : 2 * n + 5, :]


def shifts(blk, grp, flip, turn):
    return [
        (b * grp + g, (b ^ flip) * grp + (g + turn) % grp) for b in range(blk) for g in range(grp)
    ]


def replicated(blk, grp, source, target, source_mass, target_mass):
    n, width = source.shape
    axes = ("blk", "grp")
    pieces = blk * grp
    total = pieces * n
    source_sq = jnp.sum(source * source, axis=1)
    target_sq = jnp.sum(target * target, axis=1)
    lines = jnp.stack([source_mass, target_mass, -KAPPA * target_sq, source_sq, target_sq])
    lines = jnp.pad(jnp.tile(lines, (1, LANES // n)), ((0, SUB - lines.shape[0]), (0, 0)))
    own = jnp.concatenate([source, target, lines], axis=0)
    near = [own] + [lax.ppermute(own, axes, shifts(blk, grp, 0, turn)) for turn in range(1, grp)]
    near = jnp.stack(near)
    have = [near] + [lax.ppermute(near, axes, shifts(blk, grp, flip, 0)) for flip in range(2, blk, 2)]
    have = have + [lax.ppermute(part, axes, shifts(blk, grp, 1, 0)) for part in have]
    rows = own.shape[0]
    f32 = jnp.float32
    column = pltpu.VMEM((total, LANES), f32)
    line = pltpu.VMEM((SUB, total), f32)
    duals = pl.pallas_call(
        functools.partial(sinkhorn_kernel, pieces=pieces, n=n, width=width),
        in_specs=[pl.BlockSpec(memory_space=pl.ANY)] * len(have),
        out_specs=pl.BlockSpec(memory_space=pltpu.VMEM),
        out_shape=jax.ShapeDtypeStruct((SUB, LANES), f32),
        scratch_shapes=[
            pltpu.VMEM((pieces, rows, width), f32),
            pltpu.VMEM((total, 6 * width), jnp.bfloat16),
            pltpu.VMEM((total, 6 * width), jnp.bfloat16),
            pltpu.VMEM((total, total), f32),
            pltpu.VMEM((total, total), f32),
            column,
            column,
            column,
            line,
            line,
            line,
            line,
            line,
            pltpu.SMEM((2,), jnp.int32),
            pltpu.SemaphoreType.DMA((len(have),)),
        ],
        compiler_params=pltpu.CompilerParams(vmem_limit_bytes=60 * 2**20),
        name="sinkhorn",
    )(*have)
    return duals[0, :n], duals[1, :n]


def fits(mesh, n, width):
    blk, grp = mesh.shape["blk"], mesh.shape["grp"]
    total = blk * grp * n
    held = 8 * total * total + 32 * total * width
    return width == LANES and LANES % n == 0 and n % SUB == 0 and total % 256 == 0 and blk & (blk - 1) == 0 and blk > 1 and held <= VMEM_BUDGET


def solution(mesh):
    def body(source, target, source_mass, target_mass):
        if fits(mesh, *source.shape):
            return replicated(mesh.shape["blk"], mesh.shape["grp"], source, target, source_mass, target_mass)
        return per_device(source, target, source_mass, target_mass)

    return jax.shard_map(
        body,
        mesh=mesh,
        in_specs=(
            P(("blk", "grp"), None),
            P(("blk", "grp"), None),
            P(("blk", "grp")),
            P(("blk", "grp")),
        ),
        out_specs=(P(("blk", "grp")), P(("blk", "grp"))),
        check_vma=False,
    )
```
